32 devices in a mesh: pair: 8 (over y, x, core), ga: 4 (over z).
Axes of the slice: x: 2, y: 2, z: 4, core: 2. Of those that a mesh axis runs over, the one named last changes fastest.
Arguments:
- densities: bfloat16 [12288, 4096], P('pair', 'ga'), may hold values from -6 to 6
- val_band: int32 [12288], P('pair'), may hold values from 0 to 127
- cond_band: int32 [12288], P('pair'), may hold values from 0 to 255
- val_energy: float32 [128], replicated, may hold values from -12 to -1
- cond_energy: float32 [256], replicated, may hold values from 1 to 12
Outputs:
- chi: float32 [4096, 4096], P('ga', 'pair')
The draws below stay inside these ranges and needn't reach their ends.
All inputs are finite; a program needn't handle non-finite values.
Results may differ from the reference program's by a relative error of at most 0.0012.
Values may be sent and summed in bfloat16 or wider, within the bound.
A program may use at most 128 MiB of HBM per device.

```python
import math
import jax
import jax.numpy as jnp
from jax import lax

NG = 4096
NV = 128
NC = 256
P_DEV = 1536
PAIRS = 12288
N_PAIR = 8


def place_ends(array, stream_key, least, top_value):
    shape = array.shape
    index_at = [jax.random.randint(jax.random.fold_in(stream_key, axis), (), 0, shape[axis]) for axis in range(len(shape))]
    array = array.at[tuple(index_at)].set(least)
    longest = shape.index(max(shape))
    index_at[longest] = (index_at[longest] + 1) % shape[longest]
    return array.at[tuple(index_at)].set(top_value)


def steps_of(stream_key, shape, cuts, least, high):
    gain, own = 1.0, jax.random.fold_in(stream_key, 6)
    for axis_at, shards_of in cuts:
        heights = jnp.exp(jax.random.uniform(jax.random.fold_in(own, axis_at), (shards_of,), jnp.float32, least / len(cuts), high / len(cuts)))
        gain = gain * jnp.repeat(heights, shape[axis_at] // shards_of).reshape([-1 if axis == axis_at else 1 for axis in range(len(shape))])
    return gain


def gaussian(rng, shape, scale, most, shards=(), held_as=jnp.bfloat16):
    level = steps_of(rng, shape, shards, -0.22, 0.18) if shards else 1.0
    entries = jax.random.normal(rng, shape, jnp.float32) * scale * level
    return jnp.minimum(jnp.maximum(entries, -most), most).astype(held_as)


def setup_inputs(seed: int = 0) -> dict:
    arg_keys = jax.random.split(jax.random.key(seed), 6)
    return {
        "densities": gaussian(arg_keys[0], (PAIRS, NG), 1.0, 6.0, ((0, 8), (1, 4))),
        "val_band": place_ends(jax.random.randint(arg_keys[1], (PAIRS,), 0, NV), jax.random.fold_in(arg_keys[1], 1), 0, NV - 1).astype(jnp.int32),
        "cond_band": place_ends(jax.random.randint(arg_keys[2], (PAIRS,), 0, NC), jax.random.fold_in(arg_keys[2], 1), 0, NC - 1).astype(jnp.int32),
        "val_energy": jnp.clip(jax.random.uniform(arg_keys[3], (NV,), jnp.float32, -12.0, -1.0), -12.0, -1.0),
        "cond_energy": jnp.clip(jax.random.uniform(arg_keys[4], (NC,), jnp.float32, 1.0, 12.0), 1.0, 12.0),
    }


def reference(densities, val_band, cond_band, val_energy, cond_energy):
    gap = val_energy[val_band] - cond_energy[cond_band]
    weight = 4.0 / (gap * math.sqrt(PAIRS))
    scaled = (weight[:, None] * densities.astype(jnp.float32)).astype(jnp.bfloat16)
    left_groups = scaled.reshape(N_PAIR, P_DEV, NG)
    right_groups = densities.reshape(N_PAIR, P_DEV, NG)

    def add_group(total, pieces):
        left, right = pieces
        partial_value = lax.dot_general(left, right, (((0,), (0,)), ((), ())), preferred_element_type=jnp.float32)
        return (total + partial_value, None)
    total, unused = lax.scan(add_group, jnp.zeros((NG, NG), jnp.float32), (left_groups, right_groups))
    return total
```

```python
import math

import jax
import jax.numpy as jnp
from jax import lax
from jax.sharding import PartitionSpec as P

CHUNKS = 2
WIRE = jnp.float16


def lookup(bands, table):
    levels = lax.broadcasted_iota(jnp.int32, (1, table.shape[0]), 1)
    onehot = (bands[:, None] == levels).astype(jnp.float32)
    return jnp.sum(onehot * table[None, :], axis=1)


def weights(densities, val_band, cond_band, val_energy, cond_energy):
    pairs_total = densities.shape[0] * lax.axis_size("pair")
    gap = lookup(val_band, val_energy) - lookup(cond_band, cond_energy)
    return 4.0 / (gap * math.sqrt(pairs_total))


def scale(weight, block):
    return (weight[:, None] * block.astype(jnp.float32)).astype(jnp.bfloat16)


def contract(left, right):
    return lax.dot_general(
        left, right, (((0,), (0,)), ((), ())), preferred_element_type=jnp.float32
    )


def gather_all(densities, *bands):
    scaled = scale(weights(densities, *bands), densities)
    gathered = lax.all_gather(densities, "ga", axis=1, tiled=True)
    owned = lax.psum_scatter(
        contract(gathered, scaled), "pair", scatter_dimension=0, tiled=True
    )
    return owned.T


PLANES, SQUARE = 4, 2
INNER = {1: 2, 2: 1}


def move(array, target):
    perm = []
    for y in range(SQUARE):
        for x in range(SQUARE):
            for core in range(2):
                for plane in range(PLANES):
                    to = target(y, x, core, plane)
                    if to is not None:
                        v, u, c, z = to
                        here = ((y * SQUARE + x) * 2 + core) * PLANES + plane
                        perm.append((here, ((v * SQUARE + u) * 2 + c) * PLANES + z))
    return lax.ppermute(array, ("pair", "ga"), perm)


def add(a, b, dtype=WIRE):
    return (a.astype(jnp.float32) + b.astype(jnp.float32)).astype(dtype)


def reduce_to(tile, owner):
    rows, width = tile.shape[0], tile.shape[1] // 2
    core = lax.rem(lax.axis_index("pair"), 2)
    mine = lax.dynamic_slice_in_dim(tile, core * width, width, 1)
    other = lax.dynamic_slice_in_dim(tile, (1 - core) * width, width, 1)

    def swap(y, x, c, z):
        return None if owner(z) is None else (y, x, 1 - c, z)

    def along_x(y, x, c, z, late):
        if owner(z) is None:
            return None
        v, u = divmod(owner(z), SQUARE)
        return (y, u, c, z) if x != u and (not late or y == v) else None

    def along_y(y, x, c, z, late):
        if owner(z) is None:
            return None
        v, u = divmod(owner(z), SQUARE)
        return (v, x, c, z) if y != v and (not late or x == u) else None

    chip = add(mine, move(other, swap))
    upper, lower = chip[: rows // 2], chip[rows // 2 :]
    upper = add(upper, move(upper, lambda *at: along_x(*at, False)))
    lower = add(lower, move(lower, lambda *at: along_y(*at, False)))
    upper = add(upper, move(upper, lambda *at: along_y(*at, True)), jnp.float32)
    lower = add(lower, move(lower, lambda *at: along_x(*at, True)), jnp.float32)
    return jnp.concatenate([upper, lower], axis=0)


def line_of_four(densities, *bands):
    weight = weights(densities, *bands)
    rows = densities.shape[1]
    half = rows // 2
    wide = half // CHUNKS
    mine = [
        jnp.concatenate(
            [densities[:, h * half + j * wide : h * half + (j + 1) * wide] for h in range(2)],
            axis=1,
        )
        for j in range(CHUNKS)
    ]

    def partner(y, x, c, z):
        return (y, x, c, z ^ 1)

    def across(y, x, c, z):
        return (y, x, c, INNER[z]) if z in INNER else None

    def outward(y, x, c, z):
        return (y, x, c, z ^ 1) if z in INNER else None

    near = [move(block, partner) for block in mine]
    far = [move(block, across) for block in mine]
    farther = [move(block, across) for block in near]

    scaled = scale(weight, densities)
    scaled_near = jnp.concatenate([scale(weight, block) for block in near], axis=1)

    def ours(blocks, owner):
        parts = [reduce_to(contract(scaled, b).astype(WIRE), owner) for b in blocks]
        return jnp.concatenate(parts, axis=1)

    def both(blocks, owner):
        home, away = [], []
        for b in blocks:
            tile = jnp.concatenate(
                [contract(scaled_near, b).astype(WIRE), contract(scaled, b).astype(WIRE)], axis=0
            )
            total = reduce_to(tile, owner)
            sent = total[:rows].astype(WIRE)
            away.append(move(sent, outward))
            home.append(total[rows:])
        away = jnp.concatenate(away, axis=1).astype(jnp.float32)
        away = away.reshape(CHUNKS, 2, wide, half).transpose(1, 0, 2, 3).reshape(rows, half)
        return jnp.concatenate(home, axis=1), away

    own = ours(mine, lambda z: z)
    next_to = ours(near, lambda z: z ^ 1)
    home_far, away_far = both(far, lambda z: INNER.get(z))
    home_farther, away_farther = both(farther, lambda z: INNER[z] ^ 1 if z in INNER else None)

    plane = lax.axis_index("ga")
    chip = lax.axis_index("pair") // 2
    inner = (plane == 1) | (plane == 2)
    opposite = jnp.where(plane < 2, 2, 1)
    beyond = jnp.where(plane < 2, 3, 0)
    result = jnp.where(chip == plane, own, next_to)
    result = jnp.where(chip == opposite, jnp.where(inner, home_far, away_far), result)
    return jnp.where(chip == beyond, jnp.where(inner, home_farther, away_farther), result)


def solution(mesh):
    placed = (P("pair", "ga"), P("pair"), P("pair"), P(), P())
    square = mesh.shape["ga"] == PLANES and mesh.shape["pair"] == 2 * SQUARE**2
    return jax.shard_map(
        line_of_four if square else gather_all,
        mesh=mesh,
        in_specs=placed,
        out_specs=P("ga", "pair"),
        check_vma=False,
    )
```

```python
import math

import jax
import jax.numpy as jnp
from jax import lax
from jax.sharding import PartitionSpec as P


CHUNKS = 2
WIRE = jnp.float16


def lookup(bands, table):
    levels = lax.broadcasted_iota(jnp.int32, (1, table.shape[0]), 1)
    onehot = (bands[:, None] == levels).astype(jnp.float32)
    return jnp.sum(onehot * table[None, :], axis=1)


def weights(densities, val_band, cond_band, val_energy, cond_energy):
    pairs_total = densities.shape[0] * lax.axis_size("pair")
    gap = lookup(val_band, val_energy) - lookup(cond_band, cond_energy)
    return 4.0 / (gap * math.sqrt(pairs_total))


def scale(weight, block):
    return (weight[:, None] * block.astype(jnp.float32)).astype(jnp.bfloat16)


def contract(left, right):
    return lax.dot_general(
        left, right, (((0,), (0,)), ((), ())), preferred_element_type=jnp.float32
    )


def gather_all(densities, *bands):
    scaled = scale(weights(densities, *bands), densities)
    gathered = lax.all_gather(densities, "ga", axis=1, tiled=True)
    owned = lax.psum_scatter(
        contract(gathered, scaled), "pair", scatter_dimension=0, tiled=True
    )
    return owned.T


PLANES, SQUARE = 4, 2
INNER = {1: 2, 2: 1}


def move(array, target):
    perm = []
    for y in range(SQUARE):
        for x in range(SQUARE):
            for core in range(2):
                for plane in range(PLANES):
                    to = target(y, x, core, plane)
                    if to is not None:
                        v, u, c, z = to
                        here = ((y * SQUARE + x) * 2 + core) * PLANES + plane
                        perm.append((here, ((v * SQUARE + u) * 2 + c) * PLANES + z))
    return lax.ppermute(array, ("pair", "ga"), perm)


def add(a, b, dtype=WIRE):
    return (a.astype(jnp.float32) + b.astype(jnp.float32)).astype(dtype)


def reduce_to(tile, owner):
    rows, width = tile.shape[0], tile.shape[1] // 2
    core = lax.rem(lax.axis_index("pair"), 2)
    mine = lax.dynamic_slice_in_dim(tile, core * width, width, 1)
    other = lax.dynamic_slice_in_dim(tile, (1 - core) * width, width, 1)

    def swap(y, x, c, z):
        return None if owner(z) is None else (y, x, 1 - c, z)

    def along_x(y, x, c, z, late):
        if owner(z) is None:
            return None
        v, u = divmod(owner(z), SQUARE)
        return (y, u, c, z) if x != u and (not late or y == v) else None

    def along_y(y, x, c, z, late):
        if owner(z) is None:
            return None
        v, u = divmod(owner(z), SQUARE)
        return (v, x, c, z) if y != v and (not late or x == u) else None

    chip = add(mine, move(other, swap))
    upper, lower = chip[: rows // 2], chip[rows // 2 :]
    upper = add(upper, move(upper, lambda *at: along_x(*at, False)))
    lower = add(lower, move(lower, lambda *at: along_y(*at, False)))

    def finish(upper, lower):
        top = add(upper, move(upper, lambda *at: along_y(*at, True)), jnp.float32)
        low = add(lower, move(lower, lambda *at: along_x(*at, True)), jnp.float32)
        return jnp.concatenate([top, low], axis=0)

    return (upper, lower), finish


def line_of_four(densities, *bands):
    return line_of_four_body(densities, *bands)


def line_of_four_body(densities, *bands):
    weight = weights(densities, *bands)
    rows = densities.shape[1]
    half = rows // 2
    wide = half // CHUNKS
    mine = [
        jnp.concatenate(
            [densities[:, h * half + j * wide : h * half + (j + 1) * wide] for h in range(2)],
            axis=1,
        )
        for j in range(CHUNKS)
    ]

    def partner(y, x, c, z):
        return (y, x, c, z ^ 1)

    def across(y, x, c, z):
        return (y, x, c, INNER[z]) if z in INNER else None

    def outward(y, x, c, z):
        return (y, x, c, z ^ 1) if z in INNER else None

    near, farther = [], []
    for j in range(CHUNKS):
        near.append(move(mine[j], partner))
        if j == 0:
            far = move(densities, across)
    for j in range(CHUNKS):
        farther.append(move(near[j], across))

    scaled = scale(weight, densities)
    sums, finish = reduce_to(contract(scaled, densities).astype(WIRE), lambda z: z)
    own = finish(*sums)
    own, near = lax.optimization_barrier((own, near))
    scaled_near = [scale(weight, block) for block in near]

    def natural(tiles):
        return jnp.concatenate(
            [t[:, h * wide : (h + 1) * wide] for h in range(2) for t in tiles], axis=1
        )

    def both(block, owner):
        tile = jnp.concatenate(
            [contract(s, block).astype(WIRE) for s in scaled_near]
            + [contract(scaled, block).astype(WIRE)],
            axis=0,
        )
        return reduce_to(tile, owner)

    def split(total):
        away = move(total[:rows].astype(WIRE), outward)
        return total[rows:], away

    def in_order(away):
        away = away.astype(jnp.float32)
        return away.reshape(CHUNKS, 2, wide, half).transpose(1, 0, 2, 3).reshape(rows, half)

    opp, finish_opp = both(far, INNER.get)
    tile = natural([contract(scaled, b).astype(WIRE) for b in near])
    sums, finish_next = reduce_to(tile, lambda z: z ^ 1)
    opp, sums, farther = lax.optimization_barrier((opp, sums, farther))
    home_far, away_far = split(finish_opp(*opp))
    away_far = in_order(away_far)
    next_to = finish_next(*sums)
    last = []
    for j in range(CHUNKS):
        sums, finish = both(farther[j], lambda z: INNER[z] ^ 1 if z in INNER else None)
        last.append(split(finish(*sums)))
    home_farther = jnp.concatenate([home for home, _ in last], axis=1)
    away_farther = in_order(jnp.concatenate([away for _, away in last], axis=1))

    plane = lax.axis_index("ga")
    chip = lax.axis_index("pair") // 2
    inner = (plane == 1) | (plane == 2)
    opposite = jnp.where(plane < 2, 2, 1)
    beyond = jnp.where(plane < 2, 3, 0)
    result = jnp.where(chip == plane, own, next_to)
    result = jnp.where(chip == opposite, jnp.where(inner, home_far, away_far), result)
    return jnp.where(chip == beyond, jnp.where(inner, home_farther, away_farther), result)


def solution(mesh):
    placed = (P("pair", "ga"), P("pair"), P("pair"), P(), P())
    square = mesh.shape["ga"] == PLANES and mesh.shape["pair"] == 2 * SQUARE**2
    return jax.shard_map(
        line_of_four if square else gather_all,
        mesh=mesh,
        in_specs=placed,
        out_specs=P("ga", "pair"),
        check_vma=False,
    )
```
